32 devices in a mesh: expert: 4 (over y, core), mp: 8 (over z, x).
Axes of the slice: x: 2, y: 2, z: 4, core: 2. Of those that a mesh axis runs over, the one named last changes fastest.
Arguments:
- tokens: bfloat16 [512, 6144], P(('expert', 'mp')), may hold values from -18 to 18
- norm_gain: bfloat16 [6144], replicated, may hold values from 0.099609375 to 1.8984375
- expert_ids: int32 [512, 2], P(('expert', 'mp')), may hold values from 0 to 3, as said below
- slot_ids: int32 [512, 2], P(('expert', 'mp')), may hold values from 0 to 7, as said below
- route_weights: float32 [512, 2], P(('expert', 'mp')), may hold values from 0.1 to 1
- w_gate: bfloat16 [4, 6144, 8192], P('expert', None, 'mp'), may hold values from -0.078125 to 0.078125
- w_up: bfloat16 [4, 6144, 8192], P('expert', None, 'mp'), may hold values from -0.078125 to 0.078125
- w_down: bfloat16 [4, 8192, 6144], P('expert', 'mp'), may hold values from -0.0625 to 0.0625
Outputs:
- moe_out: bfloat16 [512, 6144], P(('expert', 'mp'))
The draws below stay inside these ranges and needn't reach their ends.
Inputs may be any that keep to these rules, and one draw needn't show every extreme that they name: `expert_ids`: each token names two different experts. Among the 16 tokens of one device (aligned blocks of rows) no expert is named more than 8 times, and on every device some expert is named exactly 8 times. `slot_ids`: within the tokens of one device, the entries that name the same expert have different slots; slots that no entry names stay empty.
All inputs are finite; a program needn't handle non-finite values.
Results may differ from the reference program's by a relative error of at most 0.015.
Values may be sent and summed in bfloat16 or wider, within the bound.
A program may use at most 128 MiB of HBM per device.

```python
import math
import jax
import jax.numpy as jnp
from jax import lax

D = 6144
FF = 8192
EXPERTS = 4
TOK_DEV = 16
CAP = 8
TOKENS = 512
N_MP = 8


def route_tables(key):
    blocks = TOKENS // TOK_DEV

    def one_block(index):
        block_key = jax.random.fold_in(key, index)
        key_busy, key_pool, key_slot, key_order = jax.random.split(block_key, 4)
        busiest = jax.random.randint(key_busy, (), 0, EXPERTS)
        labels = jnp.arange((EXPERTS - 1) * CAP, dtype=jnp.int32) // CAP
        others = labels + (labels >= busiest).astype(jnp.int32)
        mixing = jax.random.permutation(key_pool, (EXPERTS - 1) * CAP)
        chosen = others[mixing[:2 * TOK_DEV - CAP]]
        sequence = jnp.sort(jnp.concatenate([jnp.full((CAP,), busiest, jnp.int32), chosen]))
        below = jnp.sum((sequence[None, :] < sequence[:, None]).astype(jnp.int32), axis=1)
        within = jnp.arange(2 * TOK_DEV, dtype=jnp.int32) - below
        tables = jax.vmap(lambda expert: jax.random.permutation(jax.random.fold_in(key_slot, expert), CAP))(jnp.arange(EXPERTS))
        slot_sequence = tables[sequence, within].astype(jnp.int32)
        token_order = jax.random.permutation(key_order, TOK_DEV)
        chosen_ids = jnp.stack([sequence[token_order], sequence[TOK_DEV + token_order]], axis=1)
        chosen_slots = jnp.stack([slot_sequence[token_order], slot_sequence[TOK_DEV + token_order]], axis=1)
        return (chosen_ids, chosen_slots)
    all_ids, all_slots = jax.vmap(one_block)(jnp.arange(blocks))
    return (all_ids.reshape(TOKENS, 2).astype(jnp.int32), all_slots.reshape(TOKENS, 2).astype(jnp.int32))


def draw_expert_ids(key, part):
    return route_tables(jax.random.fold_in(key, 7))[0]


def draw_slot_ids(key, part):
    return route_tables(jax.random.fold_in(key, 7))[1]


def draw_tokens(key, part):
    key_base, key_scale = jax.random.split(jax.random.fold_in(key, 3))
    base = jnp.clip(jax.random.normal(key_base, (TOKENS, D), jnp.float32), -6.0, 6.0)
    scale = jnp.exp(jax.random.uniform(key_scale, (TOKENS, 1), jnp.float32, math.log(0.3), math.log(3.0)))
    return (base * scale).astype(jnp.bfloat16)


def steps_of(own_key, dims, shards, least, largest):
    factor_of, own = 1.0, jax.random.fold_in(own_key, 6)
    for axis_at, parts in shards:
        steps = jnp.exp(jax.random.uniform(jax.random.fold_in(own, axis_at), (parts,), jnp.float32, least / len(shards), largest / len(shards)))
        factor_of = factor_of * jnp.repeat(steps, dims[axis_at] // parts).reshape([-1 if axis == axis_at else 1 for axis in range(len(dims))])
    return factor_of


def normal_values(rng, extent, scale, bound, shards=(), held_as=jnp.bfloat16):
    gain = steps_of(rng, extent, shards, -0.22, 0.18) if shards else 1.0
    entries = jax.random.normal(rng, extent, jnp.float32) * scale * gain
    return jnp.minimum(jnp.maximum(entries, -bound), bound).astype(held_as)


def setup_inputs(seed: int = 0) -> dict:
    key_of = jax.random.split(jax.random.key(seed), 9)
    return {
        "tokens": draw_tokens(jax.random.fold_in(key_of[8], 71), 0),
        "norm_gain": jnp.clip(1.0 + 0.18 * jax.random.normal(key_of[1], (D,), jnp.float32), 0.099609375, 1.8984375).astype(jnp.bfloat16),
        "expert_ids": draw_expert_ids(jax.random.fold_in(key_of[8], 71), 0),
        "slot_ids": draw_slot_ids(jax.random.fold_in(key_of[8], 71), 0),
        "route_weights": jnp.clip(jnp.exp(math.log(1.0) - 2.3025851 * jax.random.uniform(key_of[4], (TOKENS, 2), jnp.float32) ** steps_of(key_of[4], (TOKENS, 2), ((0, 32),), -0.2, 0.2)), 0.1, 1.0),
        "w_gate": normal_values(key_of[5], (EXPERTS, D, FF), D ** -0.5, 0.078125, ((0, 4), (2, 8))),
        "w_up": normal_values(key_of[6], (EXPERTS, D, FF), D ** -0.5, 0.078125, ((0, 4), (2, 8))),
        "w_down": normal_values(key_of[7], (EXPERTS, FF, D), FF ** -0.5, 0.0625, ((0, 4), (1, 8))),
    }


def reference(tokens, norm_gain, expert_ids, slot_ids, route_weights, w_gate, w_up, w_down):
    values = tokens.astype(jnp.float32)
    mean_square = lax.optimization_barrier(jnp.mean(values * values, axis=1, keepdims=True))
    normed = (values * lax.rsqrt(mean_square + 1e-05) * norm_gain.astype(jnp.float32)).astype(jnp.bfloat16)
    block_index = (jnp.arange(TOKENS, dtype=jnp.int32) // TOK_DEV).astype(jnp.int32)
    row_index = (block_index[:, None] * CAP + slot_ids).astype(jnp.int32)
    expert_rows = TOKENS // TOK_DEV * CAP
    buffer = jnp.zeros((EXPERTS, expert_rows, D), jnp.bfloat16)
    filled = jnp.broadcast_to(normed[:, None, :], (TOKENS, 2, D))
    buffer = buffer.at[expert_ids, row_index].set(filled)
    share_width = FF // N_MP

    def one_expert(operands):
        block, gate_mat, up_mat, down_mat = operands
        gate_proj = jnp.dot(block, gate_mat, preferred_element_type=jnp.float32)
        up_proj = jnp.dot(block, up_mat, preferred_element_type=jnp.float32)
        hidden = (jax.nn.silu(gate_proj) * up_proj).astype(jnp.bfloat16)

        def add_share(total, index):
            first = (index * share_width).astype(jnp.int32)
            part_hidden = lax.dynamic_slice_in_dim(hidden, first, share_width, 1)
            part_down = lax.dynamic_slice_in_dim(down_mat, first, share_width, 0)
            product = jnp.dot(part_hidden, part_down, preferred_element_type=jnp.float32).astype(jnp.bfloat16)
            product = lax.optimization_barrier(product)
            return (total + product.astype(jnp.float32), None)
        start_total = jnp.zeros((expert_rows, D), jnp.float32)
        total, unused = lax.scan(add_share, start_total, jnp.arange(N_MP, dtype=jnp.int32))
        return total.astype(jnp.bfloat16)
    expert_out = lax.map(one_expert, (buffer, w_gate, w_up, w_down))
    shares = route_weights / (route_weights[:, 0:1] + route_weights[:, 1:2])
    picked = expert_out[expert_ids, row_index].astype(jnp.float32)
    mixed = lax.optimization_barrier(jnp.sum(shares[:, :, None] * picked, axis=1))
    return mixed.astype(jnp.bfloat16)
```

```python
import functools
import math
import jax
import jax.numpy as jnp
from jax import lax
from jax.experimental import pallas as pl
from jax.experimental.pallas import tpu as pltpu
from jax.sharding import PartitionSpec as P

CAP = 8
LANES = 128
VMEM_BYTES = 67000000
ORDERS = (("x", "y", "z"), ("y", "z", "x"), ("z", "x", "y"))
AXES = ("y", "z", "x")


class Place:
    def __init__(self, dims):
        self.dims = dims
        expert, mp = lax.axis_index("expert"), lax.axis_index("mp")
        self.core = lax.rem(expert, 2)
        self.at = {
            "y": lax.div(expert, 2),
            "z": lax.div(mp, dims["x"]),
            "x": lax.rem(mp, dims["x"]),
        }

    def device(self, axis=None, step=0, core=None):
        at = dict(self.at)
        if axis is not None:
            at[axis] = at[axis] + step
        core = self.core if core is None else core
        return {"expert": at["y"] * 2 + core, "mp": at["z"] * self.dims["x"] + at["x"]}

    def region(self, order, phase, where):
        found = {}
        for turn, axis in enumerate(order):
            if turn < phase:
                found[axis] = pl.ds(0, self.dims[axis])
            elif turn == phase:
                found[axis] = pl.ds(where, 1)
            else:
                found[axis] = pl.ds(self.at[axis], 1)
        return found

    def greet(self):
        barrier = pltpu.get_barrier_semaphore()
        count = 1
        pl.semaphore_signal(
            barrier, inc=1, device_id=self.device(core=1 - self.core),
            device_id_type=pl.DeviceIdType.MESH,
        )
        for axis in AXES:
            for step in (1, -1):
                there = self.inside(axis, self.at[axis] + step)
                count = count + there.astype(jnp.int32)

                @pl.when(there)
                def _():
                    pl.semaphore_signal(
                        barrier, inc=1, device_id=self.device(axis, step),
                        device_id_type=pl.DeviceIdType.MESH,
                    )

        pl.semaphore_wait(barrier, count)

    def inside(self, axis, where):
        return (where >= 0) & (where < self.dims[axis])


def remote(src, dst, send, recv, device):
    return pltpu.make_async_remote_copy(
        src_ref=src, dst_ref=dst, send_sem=send, recv_sem=recv,
        device_id=device, device_id_type=pl.DeviceIdType.MESH,
    )


def messages(dims):
    listed = []
    for phase in range(3):
        for step in range(max(dims.values()) - 1):
            for part, order in enumerate(ORDERS):
                if step < dims[order[phase]] - 1:
                    for way in (1, -1):
                        listed.append((part, phase, order[phase], step, way))
    return listed


def grouped(dims):
    groups = {}
    for number, message in enumerate(messages(dims)):
        groups.setdefault((message[1], message[3]), []).append((number,) + message)
    return groups


def gather_kernel(dims, cuts, x_ref, out_ref, own_sem, send, recv, pair_send, pair_recv):
    me = Place(dims)
    groups = grouped(dims)
    total = len(messages(dims))

    def view(part, found, core):
        first, width = cuts[part]
        return out_ref.at[
            found["y"], pl.ds(core, 1), found["z"], found["x"], :, pl.ds(first, width)
        ]

    mine = out_ref.at[me.at["y"], me.core, me.at["z"], me.at["x"]]
    own = pltpu.make_async_copy(x_ref, mine, own_sem)
    own.start()
    me.greet()
    own.wait()
    other = me.device(core=1 - me.core)
    remote(mine, mine, pair_send.at[total], pair_recv.at[total], other).start()

    def outgoing(number, part, phase, axis, step, way):
        at = me.at[axis]
        go = me.inside(axis, at + way) & me.inside(axis, at - way * step)
        block = view(part, me.region(ORDERS[part], phase, at - way * step), me.core)
        copy = remote(block, block, send.at[number], recv.at[number], me.device(axis, way))
        return go, copy

    def incoming(number, part, phase, axis, step, way, core):
        at = me.at[axis]
        origin = at - way * (step + 1)
        go = me.inside(axis, origin)
        return go, view(part, me.region(ORDERS[part], phase, origin), core)

    for key in sorted(groups):
        for message in groups[key]:
            go, copy = outgoing(*message)
            pl.when(go)(copy.start)
        for message in groups[key]:
            number = message[0]
            go, block = incoming(*message, me.core)

            @pl.when(go)
            def _():
                remote(block, block, send.at[number], recv.at[number], other).wait_recv()
                remote(
                    block, block, pair_send.at[number], pair_recv.at[number], other
                ).start()

    for key in sorted(groups):
        for message in groups[key]:
            number = message[0]
            go, copy = outgoing(*message)
            pl.when(go)(copy.wait_send)
            go, block = incoming(*message, me.core)
            _, landed = incoming(*message, 1 - me.core)

            @pl.when(go)
            def _():
                remote(
                    block, block, pair_send.at[number], pair_recv.at[number], other
                ).wait_send()
                remote(
                    landed, landed, pair_send.at[number], pair_recv.at[number], other
                ).wait_recv()

    theirs = out_ref.at[me.at["y"], 1 - me.core, me.at["z"], me.at["x"]]
    remote(mine, mine, pair_send.at[total], pair_recv.at[total], other).wait_send()
    remote(theirs, theirs, pair_send.at[total], pair_recv.at[total], other).wait_recv()


def scatter_kernel(dims, cuts, x_ref, out_ref, acc, pair, own_sem, send, recv, pair_send,
                   pair_recv, *lands):
    me = Place(dims)
    groups = grouped(dims)
    other = me.device(core=1 - me.core)

    def cut(ref, part):
        return ref.at[:, :, :, :, pl.ds(*cuts[part])]

    def own_copy(part):
        return pltpu.make_async_copy(
            x_ref.at[:, me.core, :, :, :, pl.ds(*cuts[part])], cut(acc, part), own_sem.at[part]
        )

    def pair_copy(part):
        return remote(
            x_ref.at[:, 1 - me.core, :, :, :, pl.ds(*cuts[part])], cut(pair, part),
            pair_send.at[part], pair_recv.at[part], other,
        )

    def add(part, found, land):
        first, width = cuts[part]
        sizes = [found[axis].size for axis in AXES]

        @pl.loop(0, math.prod(sizes))
        def _(unit):
            k = lax.rem(unit, sizes[2])
            j = lax.rem(lax.div(unit, sizes[2]), sizes[1])
            i = lax.div(unit, sizes[2] * sizes[1])
            where = (
                found["y"].start + i, found["z"].start + j, found["x"].start + k,
                slice(None), pl.ds(first, width),
            )
            acc[where] = (
                acc[where].astype(jnp.float32) + land(i, j, k).astype(jnp.float32)
            ).astype(acc.dtype)

    for part in range(3):
        own_copy(part).start()
    me.greet()
    for part in range(3):
        pair_copy(part).start()
    everything = {axis: pl.ds(0, dims[axis]) for axis in AXES}
    for part in range(3):
        own_copy(part).wait()
        pair_copy(part).wait_recv()
        add(part, everything, lambda i, j, k: pair[i, j, k, :, pl.ds(*cuts[part])])

    def outgoing(number, part, phase, axis, step, way):
        at = me.at[axis]
        target = at - way * (step + 1)
        go = me.inside(axis, target)
        found = me.region(ORDERS[part], phase, target)
        block = cut(acc, part).at[found["y"], found["z"], found["x"]]
        return go, remote(
            block, lands[number], send.at[number], recv.at[number], me.device(axis, -way)
        )

    for phase, step in sorted(groups, reverse=True):
        for message in groups[phase, step]:
            go, copy = outgoing(*message)
            pl.when(go)(copy.start)
        for message in groups[phase, step]:
            number, part, _, axis, _, way = message
            at = me.at[axis]
            go = me.inside(axis, at + way) & me.inside(axis, at - way * step)
            found = me.region(ORDERS[part], phase, at - way * step)
            land = lands[number]

            @pl.when(go)
            def _():
                remote(land, land, send.at[number], recv.at[number], other).wait_recv()
                add(part, found, lambda i, j, k: land[i, j, k])

    out_ref[...] = acc[me.at["y"], me.at["z"], me.at["x"]]
    for group in groups.values():
        for message in group:
            go, copy = outgoing(*message)
            pl.when(go)(copy.wait_send)
    for part in range(3):
        pair_copy(part).wait_send()


def axis_dims():
    mp = lax.axis_size("mp")
    along_z = math.gcd(mp, 4)
    return {"y": lax.axis_size("expert") // 2, "z": along_z, "x": mp // along_z}


def column_cuts(columns):
    tiles = columns // LANES
    middle = tiles * 3 // 8
    widths = (tiles - 2 * middle, middle, middle)
    starts = (0, widths[0], widths[0] + widths[1])
    return tuple((a * LANES, b * LANES) for a, b in zip(starts, widths))


def gather_all(payload):
    dims = axis_dims()
    rows, columns = payload.shape
    total = len(messages(dims))
    gathered = pl.pallas_call(
        functools.partial(gather_kernel, dims, column_cuts(columns)),
        out_shape=jax.ShapeDtypeStruct(
            (dims["y"], 2, dims["z"], dims["x"], rows, columns), payload.dtype
        ),
        in_specs=[pl.BlockSpec(memory_space=pl.ANY)],
        out_specs=pl.BlockSpec(memory_space=pltpu.VMEM),
        scratch_shapes=[
            pltpu.SemaphoreType.DMA,
            pltpu.SemaphoreType.DMA((total,)),
            pltpu.SemaphoreType.DMA((total,)),
            pltpu.SemaphoreType.DMA((total + 1,)),
            pltpu.SemaphoreType.DMA((total + 1,)),
        ],
        compiler_params=pltpu.CompilerParams(
            collective_id=0, has_side_effects=True, vmem_limit_bytes=VMEM_BYTES
        ),
        name="token_gather",
    )(payload)
    return gathered.reshape(-1, columns)


def scatter_sum(spread, rows):
    dims = axis_dims()
    columns = spread.shape[1]
    cuts = column_cuts(columns)
    listed = messages(dims)
    lands = []
    for part, phase, axis, step, way in listed:
        done = ORDERS[part][:phase]
        lands.append(
            pltpu.VMEM(
                tuple(dims[a] if a in done else 1 for a in AXES) + (rows, cuts[part][1]),
                spread.dtype,
            )
        )
    whole = (dims["y"], dims["z"], dims["x"], rows, columns)
    return pl.pallas_call(
        functools.partial(scatter_kernel, dims, cuts),
        out_shape=jax.ShapeDtypeStruct((rows, columns), spread.dtype),
        in_specs=[pl.BlockSpec(memory_space=pl.ANY)],
        out_specs=pl.BlockSpec(memory_space=pltpu.VMEM),
        scratch_shapes=[
            pltpu.VMEM(whole, spread.dtype),
            pltpu.VMEM(whole, spread.dtype),
            pltpu.SemaphoreType.DMA((3,)),
            pltpu.SemaphoreType.DMA((len(listed),)),
            pltpu.SemaphoreType.DMA((len(listed),)),
            pltpu.SemaphoreType.DMA((3,)),
            pltpu.SemaphoreType.DMA((3,)),
        ]
        + lands,
        compiler_params=pltpu.CompilerParams(
            collective_id=1, has_side_effects=True, vmem_limit_bytes=VMEM_BYTES
        ),
        name="result_scatter",
    )(spread.reshape(dims["y"], 2, dims["z"], dims["x"], rows, columns))


def local(tokens, norm_gain, expert_ids, slot_ids, route_weights, w_gate, w_up, w_down):
    tok_rows, features = tokens.shape
    blocks = lax.axis_size("expert") * lax.axis_size("mp")
    values = tokens.astype(jnp.float32)
    mean_square = jnp.mean(values * values, axis=1, keepdims=True)
    normed = (values * lax.rsqrt(mean_square + 1e-05) * norm_gain.astype(jnp.float32)).astype(
        jnp.bfloat16
    )
    shares = route_weights / (route_weights[:, 0:1] + route_weights[:, 1:2])
    share_hi = shares.astype(jnp.bfloat16)
    share_lo = (shares - share_hi.astype(jnp.float32)).astype(jnp.bfloat16)
    info = jnp.concatenate(
        [expert_ids.astype(jnp.bfloat16), slot_ids.astype(jnp.bfloat16), share_hi, share_lo], axis=1
    )
    info = jnp.pad(info, ((0, 0), (0, 128 - info.shape[1])))
    payload = jnp.concatenate([normed, info], axis=1)
    gathered = gather_all(payload)
    everyone = gathered[:, :features]
    table = gathered[:, features:].astype(jnp.float32)
    ids = table[:, 0:2].astype(jnp.int32)
    slots = table[:, 2:4].astype(jnp.int32)
    weights = table[:, 4:6] + table[:, 6:8]
    total = blocks * tok_rows
    block = lax.broadcasted_iota(jnp.int32, (total, 2), 0) // tok_rows
    place = jnp.where(ids == lax.axis_index("expert"), block * CAP + slots, -1)
    rows = lax.broadcasted_iota(jnp.int32, (blocks * CAP, total), 0)
    hit0 = rows == place[None, :, 0]
    hit1 = rows == place[None, :, 1]
    placing = (hit0 | hit1).astype(jnp.bfloat16)
    row_weight = jnp.sum(
        jnp.where(hit0, weights[None, :, 0], 0.0) + jnp.where(hit1, weights[None, :, 1], 0.0),
        axis=1,
        keepdims=True,
    )
    piece = jnp.dot(placing, everyone, preferred_element_type=jnp.float32).astype(jnp.bfloat16)
    gate_proj = jnp.dot(piece, w_gate[0], preferred_element_type=jnp.float32)
    up_proj = jnp.dot(piece, w_up[0], preferred_element_type=jnp.float32)
    hidden = (jax.nn.silu(gate_proj) * up_proj).astype(jnp.bfloat16)
    part = jnp.dot(hidden, w_down[0], preferred_element_type=jnp.float32)
    part = (part * row_weight).astype(jnp.bfloat16)
    spread = lax.dot_general(
        placing, part, (((0,), (0,)), ((), ())), preferred_element_type=jnp.float32
    ).astype(jnp.bfloat16)
    return scatter_sum(spread, tok_rows)


def solution(mesh):
    placed = (
        P(("expert", "mp"), None),
        P(),
        P(("expert", "mp"), None),
        P(("expert", "mp"), None),
        P(("expert", "mp"), None),
        P("expert", None, "mp"),
        P("expert", None, "mp"),
        P("expert", "mp", None),
    )
    return jax.shard_map(
        local, mesh=mesh, in_specs=placed, out_specs=P(("expert", "mp"), None), check_vma=False
    )
```
